32 devices in a mesh: grp: 2 (over core), tile: 16 (over z, y, x).
Axes of the slice: x: 2, y: 2, z: 4, core: 2. Of those that a mesh axis runs over, the one named last changes fastest.
Arguments:
- attn_input: bfloat16 [2048, 4096], P(('grp', 'tile')), may hold values from -9 to 9
- mlp_input: bfloat16 [2048, 4096], P(('grp', 'tile')), may hold values from -9 to 9
Outputs:
- hess_attn: float32 [16, 1024, 1024], P('tile', 'grp')
- hess_mlp: float32 [16, 1024, 1024], P('tile', 'grp')
The draws below stay inside these ranges and needn't reach their ends.
All inputs are finite; a program needn't handle non-finite values.
Results may differ from the reference program's by a relative error of at most 0.0003.
Values may be sent and summed in bfloat16 or wider, within the bound.
A program may use at most 192 MiB of HBM per device.

```python
import jax
import jax.numpy as jnp
from jax import lax

W = 4096
ROWB = 4
TOKENS = 2048
COLB = 4
RT = 1024
CT = 1024


def block_levels(rng, dims, pieces, least, largest):
    level = 1.0
    for axis_at, shards_of in pieces:
        draws = jax.random.uniform(jax.random.fold_in(jax.random.fold_in(rng, 6), axis_at), (shards_of,), jnp.float32, least / len(pieces), largest / len(pieces))
        level = level * jnp.repeat(jnp.exp(draws), dims[axis_at] // shards_of).reshape((-1,) + (1,) * (len(dims) - 1 - axis_at))
    return level


def gaussian(key, dims, width, reach, cuts=(), dtype=jnp.bfloat16):
    array = jax.random.normal(key, dims, jnp.float32) * width
    if len(cuts) > 0:
        array = block_levels(key, dims, cuts, -0.22, 0.18) * array
    return jnp.clip(array, min=-reach, max=reach).astype(dtype)


def setup_inputs(seed: int = 0) -> dict:
    key_of = jax.random.split(jax.random.key(seed), 3)
    return {
        "attn_input": gaussian(key_of[0], (TOKENS, W), 1.5, 9.0, ((0, 32),)),
        "mlp_input": gaussian(key_of[1], (TOKENS, W), 1.5, 9.0, ((0, 32),)),
    }


def hessian_tiles(inputs):
    widened = inputs.astype(jnp.float32)
    gram_full = jnp.dot(widened.T, widened, precision=lax.Precision.HIGHEST)
    gram_full = gram_full * (2.0 / TOKENS)
    tiled = gram_full.reshape(ROWB, RT, COLB, CT).transpose(0, 2, 1, 3)
    return tiled.reshape(ROWB * COLB, RT, CT)


def reference(attn_input, mlp_input):
    return (hessian_tiles(attn_input), hessian_tiles(mlp_input))
```

```python
import functools

import jax
import jax.numpy as jnp
from jax import lax
from jax.experimental import pallas as pl
from jax.experimental.pallas import tpu as pltpu
from jax.sharding import PartitionSpec as P

ROWB = 4
TOKB = 32
MESH = pl.DeviceIdType.MESH
LAG = 4


def tile_first(inputs, tile_count):
    tok_rows, feat_width = inputs.shape
    col_blocks = tile_count // ROWB
    row_width = feat_width // ROWB
    col_width = feat_width // col_blocks

    def accumulate(turn_idx, partial_value):
        tok_block = lax.dynamic_slice_in_dim(inputs, turn_idx * TOKB, TOKB, 0)
        row_parts = tok_block.reshape(TOKB, ROWB, row_width).transpose(1, 0, 2)
        row_send = jnp.repeat(row_parts, col_blocks, axis=0)
        col_parts = tok_block.reshape(TOKB, col_blocks, col_width).transpose(1, 0, 2)
        col_send = jnp.tile(col_parts, (ROWB, 1, 1))
        rows_in, cols_in = (
            lax.all_to_all(row_send, "tile", split_axis=0, concat_axis=0, tiled=True),
            lax.all_to_all(col_send, "tile", split_axis=0, concat_axis=0, tiled=True),
        )
        rows_flat = rows_in.reshape(tile_count * TOKB, row_width)
        cols_flat = cols_in.reshape(tile_count * TOKB, col_width)
        return partial_value + lax.dot_general(
            rows_flat, cols_flat, (((0,), (0,)), ((), ())), preferred_element_type=jnp.float32
        )

    partial_value = lax.fori_loop(
        0, tok_rows // TOKB, accumulate, jnp.zeros((row_width, col_width), jnp.float32)
    )
    shares = lax.psum_scatter(partial_value, "grp", scatter_dimension=0, tiled=True)
    return shares[None]


def hessian_share(inputs):
    tile_count = lax.axis_size("tile")
    group_count = lax.axis_size("grp")
    norm_factor = 2.0 / (inputs.shape[0] * tile_count * group_count)
    shares = tile_first(inputs, tile_count)
    return shares * norm_factor


def ring_place(member):
    return member + (member // 2) * (1 - 2 * (member % 2))


def piece_of(home, turn):
    near = home + 1 - 2 * (home % 2)
    far = (home + 2) % ROWB
    return jnp.where(turn == 0, home, jnp.where(turn == 1, near, jnp.where(turn == 2, far, ROWB - 1 - home)))


def kernel(norm_factor, xa, xm, out_a, out_m, cbuf, dbuf, rbuf, c_recv, d_recv, r_recv, s1_send, dn_send, up_send, d_send, r_send):
    lines = planes = ROWB
    g = lax.axis_index("grp")
    t = lax.axis_index("tile")
    z, p = t // planes, t % planes
    tok, _ = xa.shape
    ct = cbuf.shape[-1]
    rh = rbuf.shape[-1]
    xs = (xa, xm)
    outs = (out_a, out_m)
    half = pl.ds(pl.multiple_of(g * rh, rh), rh)

    fwd = (ring_place(p) - ring_place(z) + planes) % planes
    bwd = (planes - fwd) % planes
    is_root = fwd == 0
    ring_fwd = ring_place((ring_place(p) + 1) % planes)
    ring_bwd = ring_place((ring_place(p) + planes - 1) % planes)

    def chip(zz, pp, gg=None):
        return (g if gg is None else gg, zz * planes + pp)

    barrier = pltpu.get_barrier_semaphore()
    pl.semaphore_signal(barrier, inc=1, device_id=chip(z, p, 1 - g), device_id_type=MESH)
    for turn in range(1, planes):
        pl.semaphore_signal(barrier, inc=1, device_id=chip(z, piece_of(p, turn)), device_id_type=MESH)

    @pl.when(z > 0)
    def _():
        pl.semaphore_signal(barrier, inc=1, device_id=chip(z - 1, p), device_id_type=MESH)

    @pl.when(z < lines - 1)
    def _():
        pl.semaphore_signal(barrier, inc=1, device_id=chip(z + 1, p), device_id_type=MESH)

    pl.semaphore_wait(barrier, planes + jnp.where(z > 0, 1, 0) + jnp.where(z < lines - 1, 1, 0))

    def s1_copy(a, turn):
        other = piece_of(p, turn)
        cols = pl.ds(pl.multiple_of(other * ct, ct), ct)
        return pltpu.make_async_remote_copy(
            src_ref=xs[a].at[:, cols], dst_ref=cbuf.at[a, z, p], send_sem=s1_send.at[a, turn - 1],
            recv_sem=c_recv.at[a, z, p], device_id=chip(z, other), device_id_type=MESH)

    def own_copy(a):
        cols = pl.ds(pl.multiple_of(p * ct, ct), ct)
        return pltpu.make_async_copy(xs[a].at[:, cols], cbuf.at[a, z, p], c_recv.at[a, z, p])

    def line_copy(a, slot, piece, down):
        return pltpu.make_async_remote_copy(
            src_ref=cbuf.at[a, slot, piece], dst_ref=cbuf.at[a, slot, piece],
            send_sem=(dn_send if down else up_send).at[a, slot, piece], recv_sem=c_recv.at[a, slot, piece],
            device_id=chip(z - 1 if down else z + 1, p), device_id_type=MESH)

    def pair_copy(a, slot, piece):
        return pltpu.make_async_remote_copy(
            src_ref=cbuf.at[a, slot, piece], dst_ref=dbuf.at[a, slot, piece], send_sem=d_send.at[a, slot, piece],
            recv_sem=d_recv.at[a, slot, piece], device_id=chip(z, p, 1 - g), device_id_type=MESH)

    def ring_copy(src, a, slot, gg, piece, way):
        return pltpu.make_async_remote_copy(
            src_ref=src, dst_ref=rbuf.at[a, slot, gg, piece], send_sem=r_send.at[a, slot, gg, piece],
            recv_sem=r_recv.at[a, slot, gg, piece],
            device_id=chip(z, ring_fwd * (1 - way) + ring_bwd * way), device_id_type=MESH)

    def landed(ref, sem):
        pltpu.make_async_copy(ref, ref, sem).wait()

    for a in range(2):
        own_copy(a).start()
        for turn in range(1, planes):
            s1_copy(a, turn).start()
    for out in outs:
        out[...] = jnp.zeros_like(out)

    def root_feed(src, a, slot, gg, piece, turn):
        @pl.when(is_root)
        def _():
            pltpu.make_async_copy(src, rbuf.at[a, slot, gg, piece], r_recv.at[a, slot, gg, piece]).start()
            ring_copy(src, a, slot, gg, piece, (turn + gg) % 2).start()

    def each_slot(k, action):
        dist, a, turn = k // (2 * planes), (k // planes) % 2, k % planes
        high, low = z + dist, z - dist

        @pl.when((k >= 0) & (k < 2 * planes * lines))
        def _():
            @pl.when(high < lines)
            def _():
                action(a, high, turn, dist, True)

            @pl.when((dist > 0) & (low >= 0))
            def _():
                action(a, low, turn, dist, False)

    def col_phase(a, slot, turn, dist, from_high):
        piece = piece_of(p, turn)
        landed(cbuf.at[a, slot, piece], c_recv.at[a, slot, piece])
        if from_high:
            @pl.when(z > 0)
            def _():
                line_copy(a, slot, piece, True).start()

            @pl.when((dist == 0) & (z < lines - 1))
            def _():
                line_copy(a, slot, piece, False).start()
        else:
            @pl.when(z < lines - 1)
            def _():
                line_copy(a, slot, piece, False).start()
        pair_copy(a, slot, piece).start()
        root_feed(cbuf.at[a, slot, piece, :, half], a, slot, g, piece, turn)

    def pair_phase(a, slot, turn, dist, from_high):
        piece = piece_of(p, turn)
        landed(dbuf.at[a, slot, piece], d_recv.at[a, slot, piece])
        root_feed(dbuf.at[a, slot, piece, :, half], a, slot, 1 - g, piece, turn)

    def row_phase(a, slot, turn, dist, from_high):
        piece = piece_of(z, turn)
        for step in range(2):
            gg = g if step == 0 else 1 - g
            landed(rbuf.at[a, slot, gg, piece], r_recv.at[a, slot, gg, piece])
            way = (turn + gg) % 2
            span = fwd * (1 - way) + bwd * way

            @pl.when((span > 0) & (span < planes - 1))
            def _():
                ring_copy(rbuf.at[a, slot, gg, piece], a, slot, gg, piece, way).start()

        @pl.when(turn == planes - 1)
        def _():
            for arr in range(2):
                @pl.when(a == arr)
                def _():
                    total = outs[arr]
                    for cols, gg in ((cbuf, g), (dbuf, 1 - g)):
                        total[...] += lax.dot_general(
                            rbuf[arr, slot, gg].reshape(planes * tok, rh),
                            cols[arr, slot].reshape(planes * tok, ct),
                            (((0,), (0,)), ((), ())), preferred_element_type=jnp.float32)

    def step(k, carry):
        each_slot(k, col_phase)
        each_slot(k - 1, pair_phase)
        each_slot(k - LAG, row_phase)
        return carry

    lax.fori_loop(0, 2 * planes * lines + LAG, step, 0)

    for a in range(2):
        for turn in range(1, planes):
            s1_copy(a, turn).wait_send()

    def finish(a, slot, turn, dist, from_high):
        piece = piece_of(p, turn)
        if from_high:
            @pl.when(z > 0)
            def _():
                line_copy(a, slot, piece, True).wait_send()

            @pl.when((dist == 0) & (z < lines - 1))
            def _():
                line_copy(a, slot, piece, False).wait_send()
        else:
            @pl.when(z < lines - 1)
            def _():
                line_copy(a, slot, piece, False).wait_send()
        pair_copy(a, slot, piece).wait_send()
        row_piece = piece_of(z, turn)
        for gg in range(2):
            way = (turn + gg) % 2
            span = fwd * (1 - way) + bwd * way

            @pl.when(span < planes - 1)
            def _():
                ring_copy(rbuf.at[a, slot, gg, row_piece], a, slot, gg, row_piece, way).wait_send()

    def finish_step(k, carry):
        each_slot(k, finish)
        return carry

    lax.fori_loop(0, 2 * planes * lines, finish_step, 0)
    for out in outs:
        out[...] = out[...] * norm_factor


def fused(attn_input, mlp_input):
    groups, tiles = lax.axis_size("grp"), lax.axis_size("tile")
    tok, width = attn_input.shape
    ct, rh = width // ROWB, width // ROWB // groups
    norm_factor = 2.0 / (tok * tiles * groups)
    dma = pltpu.SemaphoreType.DMA
    cell = (2, ROWB, ROWB)
    hess = pl.pallas_call(
        functools.partial(kernel, norm_factor),
        out_shape=[jax.ShapeDtypeStruct((rh, ct), jnp.float32)] * 2,
        in_specs=[pl.BlockSpec(memory_space=pl.ANY)] * 2,
        out_specs=[pl.BlockSpec(memory_space=pltpu.VMEM)] * 2,
        scratch_shapes=[
            pltpu.VMEM(cell + (tok, ct), jnp.bfloat16),
            pltpu.VMEM(cell + (tok, ct), jnp.bfloat16),
            pltpu.VMEM((2, ROWB, groups, ROWB, tok, rh), jnp.bfloat16),
            dma(cell), dma(cell), dma((2, ROWB, groups, ROWB)),
            dma((2, ROWB - 1)), dma(cell), dma(cell), dma(cell), dma((2, ROWB, groups, ROWB)),
        ],
        compiler_params=pltpu.CompilerParams(collective_id=0, has_side_effects=True, vmem_limit_bytes=48 * 1024 * 1024),
    )(attn_input, mlp_input)
    return hess[0][None], hess[1][None]


def body(attn_input, mlp_input):
    if lax.axis_size("grp") == 2 and lax.axis_size("tile") == ROWB * ROWB:
        return fused(attn_input, mlp_input)
    return (hessian_share(attn_input), hessian_share(mlp_input))


def solution(mesh):
    in_specs = (P(("grp", "tile"), None), P(("grp", "tile"), None))
    out_specs = (P("tile", "grp", None), P("tile", "grp", None))
    return jax.shard_map(body, mesh=mesh, in_specs=in_specs, out_specs=out_specs, check_vma=False)
```

```python
import functools

import jax
import jax.numpy as jnp
from jax import lax
from jax.experimental import pallas as pl
from jax.experimental.pallas import tpu as pltpu
from jax.sharding import PartitionSpec as P

ROWB = 4
TOKB = 32
MESH = pl.DeviceIdType.MESH
HOP = 3
LAG = 1 + HOP * (ROWB - 1)


def tile_first(inputs, tile_count):
    tok_rows, feat_width = inputs.shape
    col_blocks = tile_count // ROWB
    row_width = feat_width // ROWB
    col_width = feat_width // col_blocks

    def accumulate(turn_idx, partial_value):
        tok_block = lax.dynamic_slice_in_dim(inputs, turn_idx * TOKB, TOKB, 0)
        row_parts = tok_block.reshape(TOKB, ROWB, row_width).transpose(1, 0, 2)
        row_send = jnp.repeat(row_parts, col_blocks, axis=0)
        col_parts = tok_block.reshape(TOKB, col_blocks, col_width).transpose(1, 0, 2)
        col_send = jnp.tile(col_parts, (ROWB, 1, 1))
        rows_in, cols_in = (
            lax.all_to_all(row_send, "tile", split_axis=0, concat_axis=0, tiled=True),
            lax.all_to_all(col_send, "tile", split_axis=0, concat_axis=0, tiled=True),
        )
        rows_flat = rows_in.reshape(tile_count * TOKB, row_width)
        cols_flat = cols_in.reshape(tile_count * TOKB, col_width)
        return partial_value + lax.dot_general(
            rows_flat, cols_flat, (((0,), (0,)), ((), ())), preferred_element_type=jnp.float32
        )

    partial_value = lax.fori_loop(
        0, tok_rows // TOKB, accumulate, jnp.zeros((row_width, col_width), jnp.float32)
    )
    shares = lax.psum_scatter(partial_value, "grp", scatter_dimension=0, tiled=True)
    return shares[None]


def hessian_share(inputs):
    tile_count = lax.axis_size("tile")
    group_count = lax.axis_size("grp")
    norm_factor = 2.0 / (inputs.shape[0] * tile_count * group_count)
    shares = tile_first(inputs, tile_count)
    return shares * norm_factor


def ring_place(member):
    return member + (member // 2) * (1 - 2 * (member % 2))


def piece_of(home, turn):
    near = home + 1 - 2 * (home % 2)
    far = (home + 2) % ROWB
    return jnp.where(turn == 0, home, jnp.where(turn == 1, near, jnp.where(turn == 2, far, ROWB - 1 - home)))


def kernel(norm_factor, xa, xm, out_a, out_m, cbuf, dbuf, rbuf, c_recv, d_recv, r_recv, s1_send, dn_send, up_send, d_send, r_send):
    lines = planes = ROWB
    g = lax.axis_index("grp")
    t = lax.axis_index("tile")
    z, p = t // planes, t % planes
    tok, _ = xa.shape
    ct = cbuf.shape[-1]
    rh = rbuf.shape[-1]
    xs = (xa, xm)
    outs = (out_a, out_m)
    half = pl.ds(pl.multiple_of(g * rh, rh), rh)

    fwd = (ring_place(p) - ring_place(z) + planes) % planes
    bwd = (planes - fwd) % planes
    is_root = fwd == 0
    ring_fwd = ring_place((ring_place(p) + 1) % planes)
    ring_bwd = ring_place((ring_place(p) + planes - 1) % planes)

    def chip(zz, pp, gg=None):
        return (g if gg is None else gg, zz * planes + pp)

    barrier = pltpu.get_barrier_semaphore()
    pl.semaphore_signal(barrier, inc=1, device_id=chip(z, p, 1 - g), device_id_type=MESH)
    for turn in range(1, planes):
        pl.semaphore_signal(barrier, inc=1, device_id=chip(z, piece_of(p, turn)), device_id_type=MESH)

    @pl.when(z > 0)
    def _():
        pl.semaphore_signal(barrier, inc=1, device_id=chip(z - 1, p), device_id_type=MESH)

    @pl.when(z < lines - 1)
    def _():
        pl.semaphore_signal(barrier, inc=1, device_id=chip(z + 1, p), device_id_type=MESH)

    pl.semaphore_wait(barrier, planes + jnp.where(z > 0, 1, 0) + jnp.where(z < lines - 1, 1, 0))

    def s1_copy(a, turn):
        other = piece_of(p, turn)
        cols = pl.ds(pl.multiple_of(other * ct, ct), ct)
        return pltpu.make_async_remote_copy(
            src_ref=xs[a].at[:, cols], dst_ref=cbuf.at[a, z, p], send_sem=s1_send.at[a, turn - 1],
            recv_sem=c_recv.at[a, z, p], device_id=chip(z, other), device_id_type=MESH)

    def own_copy(a):
        cols = pl.ds(pl.multiple_of(p * ct, ct), ct)
        return pltpu.make_async_copy(xs[a].at[:, cols], cbuf.at[a, z, p], c_recv.at[a, z, p])

    def line_copy(a, slot, piece, down):
        return pltpu.make_async_remote_copy(
            src_ref=cbuf.at[a, slot, piece], dst_ref=cbuf.at[a, slot, piece],
            send_sem=(dn_send if down else up_send).at[a, slot, piece], recv_sem=c_recv.at[a, slot, piece],
            device_id=chip(z - 1 if down else z + 1, p), device_id_type=MESH)

    def pair_copy(a, slot, piece):
        return pltpu.make_async_remote_copy(
            src_ref=cbuf.at[a, slot, piece], dst_ref=dbuf.at[a, slot, piece], send_sem=d_send.at[a, slot, piece],
            recv_sem=d_recv.at[a, slot, piece], device_id=chip(z, p, 1 - g), device_id_type=MESH)

    def ring_copy(src, a, slot, gg, piece, way):
        return pltpu.make_async_remote_copy(
            src_ref=src, dst_ref=rbuf.at[a, slot, gg, piece], send_sem=r_send.at[a, slot, gg, piece],
            recv_sem=r_recv.at[a, slot, gg, piece],
            device_id=chip(z, ring_fwd * (1 - way) + ring_bwd * way), device_id_type=MESH)

    def landed(ref, sem):
        pltpu.make_async_copy(ref, ref, sem).wait()

    for a in range(2):
        own_copy(a).start()
        for turn in range(1, planes):
            s1_copy(a, turn).start()
    for out in outs:
        out[...] = jnp.zeros_like(out)

    def root_feed(src, a, slot, gg, piece, turn):
        @pl.when(is_root)
        def _():
            pltpu.make_async_copy(src, rbuf.at[a, slot, gg, piece], r_recv.at[a, slot, gg, piece]).start()
            ring_copy(src, a, slot, gg, piece, (turn + gg) % 2).start()

    def each_slot(k, action):
        dist, a, turn = k // (2 * planes), (k // planes) % 2, k % planes
        high, low = z + dist, z - dist

        @pl.when((k >= 0) & (k < 2 * planes * lines))
        def _():
            @pl.when(high < lines)
            def _():
                action(a, high, turn, dist, True)

            @pl.when((dist > 0) & (low >= 0))
            def _():
                action(a, low, turn, dist, False)

    def col_phase(a, slot, turn, dist, from_high):
        piece = piece_of(p, turn)
        landed(cbuf.at[a, slot, piece], c_recv.at[a, slot, piece])
        if from_high:
            @pl.when(z > 0)
            def _():
                line_copy(a, slot, piece, True).start()

            @pl.when((dist == 0) & (z < lines - 1))
            def _():
                line_copy(a, slot, piece, False).start()
        else:
            @pl.when(z < lines - 1)
            def _():
                line_copy(a, slot, piece, False).start()
        pair_copy(a, slot, piece).start()
        root_feed(cbuf.at[a, slot, piece, :, half], a, slot, g, piece, turn)

    def pair_phase(a, slot, turn, dist, from_high):
        piece = piece_of(p, turn)
        landed(dbuf.at[a, slot, piece], d_recv.at[a, slot, piece])
        root_feed(dbuf.at[a, slot, piece, :, half], a, slot, 1 - g, piece, turn)

    def row_phase(way, span):
        def action(a, slot, turn, dist, from_high):
            piece = piece_of(z, turn)
            gg = (turn + way) % 2
            landed(rbuf.at[a, slot, gg, piece], r_recv.at[a, slot, gg, piece])

            @pl.when((span > 0) & (span < planes - 1))
            def _():
                ring_copy(rbuf.at[a, slot, gg, piece], a, slot, gg, piece, way).start()

        return action

    def multiply(a, slot, turn, dist, from_high):
        @pl.when(turn == planes - 1)
        def _():
            for arr in range(2):
                @pl.when(a == arr)
                def _():
                    total = outs[arr]
                    for cols, gg in ((cbuf, g), (dbuf, 1 - g)):
                        total[...] += lax.dot_general(
                            rbuf[arr, slot, gg].reshape(planes * tok, rh),
                            cols[arr, slot].reshape(planes * tok, ct),
                            (((0,), (0,)), ((), ())), preferred_element_type=jnp.float32)

    def step(k, carry):
        each_slot(k, col_phase)
        each_slot(k - 1, pair_phase)
        each_slot(k - 1 - HOP * jnp.where(fwd == 0, 1, fwd), row_phase(0, fwd))
        each_slot(k - 1 - HOP * jnp.where(bwd == 0, 1, bwd), row_phase(1, bwd))
        each_slot(k - LAG, multiply)
        return carry

    lax.fori_loop(0, 2 * planes * lines + LAG, step, 0)

    for a in range(2):
        for turn in range(1, planes):
            s1_copy(a, turn).wait_send()

    def finish(a, slot, turn, dist, from_high):
        piece = piece_of(p, turn)
        if from_high:
            @pl.when(z > 0)
            def _():
                line_copy(a, slot, piece, True).wait_send()

            @pl.when((dist == 0) & (z < lines - 1))
            def _():
                line_copy(a, slot, piece, False).wait_send()
        else:
            @pl.when(z < lines - 1)
            def _():
                line_copy(a, slot, piece, False).wait_send()
        pair_copy(a, slot, piece).wait_send()
        row_piece = piece_of(z, turn)
        for gg in range(2):
            way = (turn + gg) % 2
            span = fwd * (1 - way) + bwd * way

            @pl.when(span < planes - 1)
            def _():
                ring_copy(rbuf.at[a, slot, gg, row_piece], a, slot, gg, row_piece, way).wait_send()

    def finish_step(k, carry):
        each_slot(k, finish)
        return carry

    lax.fori_loop(0, 2 * planes * lines, finish_step, 0)
    for out in outs:
        out[...] = out[...] * norm_factor


def fused(attn_input, mlp_input):
    groups, tiles = lax.axis_size("grp"), lax.axis_size("tile")
    tok, width = attn_input.shape
    ct, rh = width // ROWB, width // ROWB // groups
    norm_factor = 2.0 / (tok * tiles * groups)
    dma = pltpu.SemaphoreType.DMA
    cell = (2, ROWB, ROWB)
    hess = pl.pallas_call(
        functools.partial(kernel, norm_factor),
        out_shape=[jax.ShapeDtypeStruct((rh, ct), jnp.float32)] * 2,
        in_specs=[pl.BlockSpec(memory_space=pl.ANY)] * 2,
        out_specs=[pl.BlockSpec(memory_space=pltpu.VMEM)] * 2,
        scratch_shapes=[
            pltpu.VMEM(cell + (tok, ct), jnp.bfloat16),
            pltpu.VMEM(cell + (tok, ct), jnp.bfloat16),
            pltpu.VMEM((2, ROWB, groups, ROWB, tok, rh), jnp.bfloat16),
            dma(cell), dma(cell), dma((2, ROWB, groups, ROWB)),
            dma((2, ROWB - 1)), dma(cell), dma(cell), dma(cell), dma((2, ROWB, groups, ROWB)),
        ],
        compiler_params=pltpu.CompilerParams(collective_id=0, has_side_effects=True, vmem_limit_bytes=48 * 1024 * 1024),
    )(attn_input, mlp_input)
    return hess[0][None], hess[1][None]


def body(attn_input, mlp_input):
    if lax.axis_size("grp") == 2 and lax.axis_size("tile") == ROWB * ROWB:
        return fused(attn_input, mlp_input)
    return (hessian_share(attn_input), hessian_share(mlp_input))


def solution(mesh):
    in_specs = (P(("grp", "tile"), None), P(("grp", "tile"), None))
    out_specs = (P("tile", "grp", None), P("tile", "grp", None))
    return jax.shard_map(body, mesh=mesh, in_specs=in_specs, out_specs=out_specs, check_vma=False)
```

```python
import jax
import jax.numpy as jnp
from jax import lax
from jax.experimental import pallas as pl
from jax.experimental.pallas import tpu as pltpu
from jax.sharding import PartitionSpec as P

ROWB = 4
TOKB = 32
MESH = pl.DeviceIdType.MESH
END_HOP = 2
MID_HOP = 4


def tile_first(inputs, tile_count):
    tok_rows, feat_width = inputs.shape
    col_blocks = tile_count // ROWB
    row_width = feat_width // ROWB
    col_width = feat_width // col_blocks

    def accumulate(turn_idx, partial_value):
        tok_block = lax.dynamic_slice_in_dim(inputs, turn_idx * TOKB, TOKB, 0)
        row_parts = tok_block.reshape(TOKB, ROWB, row_width).transpose(1, 0, 2)
        row_send = jnp.repeat(row_parts, col_blocks, axis=0)
        col_parts = tok_block.reshape(TOKB, col_blocks, col_width).transpose(1, 0, 2)
        col_send = jnp.tile(col_parts, (ROWB, 1, 1))
        rows_in, cols_in = (
            lax.all_to_all(row_send, "tile", split_axis=0, concat_axis=0, tiled=True),
            lax.all_to_all(col_send, "tile", split_axis=0, concat_axis=0, tiled=True),
        )
        rows_flat = rows_in.reshape(tile_count * TOKB, row_width)
        cols_flat = cols_in.reshape(tile_count * TOKB, col_width)
        return partial_value + lax.dot_general(
            rows_flat, cols_flat, (((0,), (0,)), ((), ())), preferred_element_type=jnp.float32
        )

    partial_value = lax.fori_loop(
        0, tok_rows // TOKB, accumulate, jnp.zeros((row_width, col_width), jnp.float32)
    )
    shares = lax.psum_scatter(partial_value, "grp", scatter_dimension=0, tiled=True)
    return shares[None]


def hessian_share(inputs):
    tile_count = lax.axis_size("tile")
    group_count = lax.axis_size("grp")
    norm_factor = 2.0 / (inputs.shape[0] * tile_count * group_count)
    shares = tile_first(inputs, tile_count)
    return shares * norm_factor


def ring_place(member):
    return member + (member // 2) * (1 - 2 * (member % 2))


def piece_of(home, turn):
    near = home + 1 - 2 * (home % 2)
    far = (home + 2) % ROWB
    return jnp.where(turn == 0, home, jnp.where(turn == 1, near, jnp.where(turn == 2, far, ROWB - 1 - home)))


def kernel(xa, xm, out_a, out_m, cbuf, dbuf, rbuf, c_recv, d_recv, r_recv, s1_send, dn_send, up_send, d_send, r_send):
    lines = planes = ROWB
    g = lax.axis_index("grp")
    t = lax.axis_index("tile")
    z, p = t // planes, t % planes
    tok, _ = xa.shape
    ct = cbuf.shape[-1]
    rh = rbuf.shape[-1]
    xs = (xa, xm)
    outs = (out_a, out_m)
    half = pl.ds(pl.multiple_of(g * rh, rh), rh)

    fwd = (ring_place(p) - ring_place(z) + planes) % planes
    bwd = (planes - fwd) % planes
    is_root = fwd == 0
    ring_fwd = ring_place((ring_place(p) + 1) % planes)
    ring_bwd = ring_place((ring_place(p) + planes - 1) % planes)

    def chip(zz, pp, gg=None):
        return (g if gg is None else gg, zz * planes + pp)

    barrier = pltpu.get_barrier_semaphore()
    pl.semaphore_signal(barrier, inc=1, device_id=chip(z, p, 1 - g), device_id_type=MESH)
    for turn in range(1, planes):
        pl.semaphore_signal(barrier, inc=1, device_id=chip(z, piece_of(p, turn)), device_id_type=MESH)

    @pl.when(z > 0)
    def _():
        pl.semaphore_signal(barrier, inc=1, device_id=chip(z - 1, p), device_id_type=MESH)

    @pl.when(z < lines - 1)
    def _():
        pl.semaphore_signal(barrier, inc=1, device_id=chip(z + 1, p), device_id_type=MESH)

    pl.semaphore_wait(barrier, planes + jnp.where(z > 0, 1, 0) + jnp.where(z < lines - 1, 1, 0))

    def s1_copy(a, turn):
        other = piece_of(p, turn)
        cols = pl.ds(pl.multiple_of(other * ct, ct), ct)
        return pltpu.make_async_remote_copy(
            src_ref=xs[a].at[:, cols], dst_ref=cbuf.at[a, z, p], send_sem=s1_send.at[a, turn - 1],
            recv_sem=c_recv.at[a, z, p], device_id=chip(z, other), device_id_type=MESH)

    def own_copy(a):
        cols = pl.ds(pl.multiple_of(p * ct, ct), ct)
        return pltpu.make_async_copy(xs[a].at[:, cols], cbuf.at[a, z, p], c_recv.at[a, z, p])

    def line_copy(a, slot, piece, down):
        return pltpu.make_async_remote_copy(
            src_ref=cbuf.at[a, slot, piece], dst_ref=cbuf.at[a, slot, piece],
            send_sem=(dn_send if down else up_send).at[a, slot, piece], recv_sem=c_recv.at[a, slot, piece],
            device_id=chip(z - 1 if down else z + 1, p), device_id_type=MESH)

    def pair_copy(a, slot, piece):
        return pltpu.make_async_remote_copy(
            src_ref=cbuf.at[a, slot, piece], dst_ref=dbuf.at[a, slot, piece], send_sem=d_send.at[a, slot, piece],
            recv_sem=d_recv.at[a, slot, piece], device_id=chip(z, p, 1 - g), device_id_type=MESH)

    def ring_copy(src, a, slot, gg, piece, way):
        return pltpu.make_async_remote_copy(
            src_ref=src, dst_ref=rbuf.at[a, slot, gg, piece], send_sem=r_send.at[a, slot, gg, piece],
            recv_sem=r_recv.at[a, slot, gg, piece],
            device_id=chip(z, ring_fwd * (1 - way) + ring_bwd * way), device_id_type=MESH)

    def landed(ref, sem):
        pltpu.make_async_copy(ref, ref, sem).wait()

    for a in range(2):
        own_copy(a).start()
    for turn in range(1, planes):
        for a in range(2):
            s1_copy(a, turn).start()
    for out in outs:
        out[...] = jnp.zeros_like(out)

    def root_feed(src, a, slot, gg, piece, turn):
        @pl.when(is_root)
        def _():
            pltpu.make_async_copy(src, rbuf.at[a, slot, gg, piece], r_recv.at[a, slot, gg, piece]).start()
            ring_copy(src, a, slot, gg, piece, (turn + gg) % 2).start()

    def each_slot(k, action):
        dist, turn, a = k // (2 * planes), (k // 2) % planes, k % 2
        high, low = z + dist, z - dist

        @pl.when((k >= 0) & (k < 2 * planes * lines))
        def _():
            @pl.when(high < lines)
            def _():
                action(a, high, turn, dist, True)

            @pl.when((dist > 0) & (low >= 0))
            def _():
                action(a, low, turn, dist, False)

    def col_phase(a, slot, turn, dist, from_high):
        piece = piece_of(p, turn)
        landed(cbuf.at[a, slot, piece], c_recv.at[a, slot, piece])
        if from_high:
            @pl.when(z > 0)
            def _():
                line_copy(a, slot, piece, True).start()

            @pl.when((dist == 0) & (z < lines - 1))
            def _():
                line_copy(a, slot, piece, False).start()
        else:
            @pl.when(z < lines - 1)
            def _():
                line_copy(a, slot, piece, False).start()
        pair_copy(a, slot, piece).start()
        root_feed(cbuf.at[a, slot, piece, :, half], a, slot, g, piece, turn)

    def pair_phase(a, slot, turn, dist, from_high):
        piece = piece_of(p, turn)
        landed(dbuf.at[a, slot, piece], d_recv.at[a, slot, piece])
        root_feed(dbuf.at[a, slot, piece, :, half], a, slot, 1 - g, piece, turn)

    def row_phase(way, span):
        def action(a, slot, turn, dist, from_high):
            piece = piece_of(z, turn)
            gg = (turn + way) % 2
            landed(rbuf.at[a, slot, gg, piece], r_recv.at[a, slot, gg, piece])

            @pl.when((span > 0) & (span < planes - 1))
            def _():
                ring_copy(rbuf.at[a, slot, gg, piece], a, slot, gg, piece, way).start()

        return action

    def multiply(a, slot, turn, dist, from_high):
        @pl.when(turn == planes - 1)
        def _():
            for arr in range(2):
                @pl.when(a == arr)
                def _():
                    total = outs[arr]
                    for cols, gg in ((cbuf, g), (dbuf, 1 - g)):
                        total[...] += lax.dot_general(
                            rbuf[arr, slot, gg].reshape(planes * tok, rh),
                            cols[arr, slot].reshape(planes * tok, ct),
                            (((0,), (0,)), ((), ())), preferred_element_type=jnp.float32)

    hop = jnp.where((z == 0) | (z == lines - 1), END_HOP, MID_HOP)
    last = 1 + hop * (planes - 1)

    def step(k, carry):
        each_slot(k, col_phase)
        each_slot(k - 1, pair_phase)
        each_slot(k - 1 - hop * jnp.where(fwd == 0, 1, fwd), row_phase(0, fwd))
        each_slot(k - 1 - hop * jnp.where(bwd == 0, 1, bwd), row_phase(1, bwd))
        each_slot(k - last, multiply)
        return carry

    lax.fori_loop(0, 2 * planes * lines + last, step, 0)

    for a in range(2):
        for turn in range(1, planes):
            s1_copy(a, turn).wait_send()

    def finish(a, slot, turn, dist, from_high):
        piece = piece_of(p, turn)
        if from_high:
            @pl.when(z > 0)
            def _():
                line_copy(a, slot, piece, True).wait_send()

            @pl.when((dist == 0) & (z < lines - 1))
            def _():
                line_copy(a, slot, piece, False).wait_send()
        else:
            @pl.when(z < lines - 1)
            def _():
                line_copy(a, slot, piece, False).wait_send()
        pair_copy(a, slot, piece).wait_send()
        row_piece = piece_of(z, turn)
        for gg in range(2):
            way = (turn + gg) % 2
            span = fwd * (1 - way) + bwd * way

            @pl.when(span < planes - 1)
            def _():
                ring_copy(rbuf.at[a, slot, gg, row_piece], a, slot, gg, row_piece, way).wait_send()

    def finish_step(k, carry):
        each_slot(k, finish)
        return carry

    lax.fori_loop(0, 2 * planes * lines, finish_step, 0)


def fused(attn_input, mlp_input):
    groups, tiles = lax.axis_size("grp"), lax.axis_size("tile")
    tok, width = attn_input.shape
    ct, rh = width // ROWB, width // ROWB // groups
    norm_factor = 2.0 / (tok * tiles * groups)
    dma = pltpu.SemaphoreType.DMA
    cell = (2, ROWB, ROWB)
    hess = pl.pallas_call(
        kernel,
        out_shape=[jax.ShapeDtypeStruct((rh, ct), jnp.float32)] * 2,
        in_specs=[pl.BlockSpec(memory_space=pl.ANY)] * 2,
        out_specs=[pl.BlockSpec(memory_space=pltpu.VMEM)] * 2,
        scratch_shapes=[
            pltpu.VMEM(cell + (tok, ct), jnp.bfloat16),
            pltpu.VMEM(cell + (tok, ct), jnp.bfloat16),
            pltpu.VMEM((2, ROWB, groups, ROWB, tok, rh), jnp.bfloat16),
            dma(cell), dma(cell), dma((2, ROWB, groups, ROWB)),
            dma((2, ROWB - 1)), dma(cell), dma(cell), dma(cell), dma((2, ROWB, groups, ROWB)),
        ],
        compiler_params=pltpu.CompilerParams(collective_id=0, has_side_effects=True, vmem_limit_bytes=48 * 1024 * 1024),
    )(attn_input, mlp_input)
    return hess[0][None] * norm_factor, hess[1][None] * norm_factor


def body(attn_input, mlp_input):
    if lax.axis_size("grp") == 2 and lax.axis_size("tile") == ROWB * ROWB:
        return fused(attn_input, mlp_input)
    return (hessian_share(attn_input), hessian_share(mlp_input))


def solution(mesh):
    in_specs = (P(("grp", "tile"), None), P(("grp", "tile"), None))
    out_specs = (P("tile", "grp", None), P("tile", "grp", None))
    return jax.shard_map(body, mesh=mesh, in_specs=in_specs, out_specs=out_specs, check_vma=False)
```
